256 devices in a mesh: radial: 64 (over x, z, core), phi: 4 (over y).
Axes of the slice: x: 4, y: 4, z: 8, core: 2. Of those that a mesh axis runs over, the one named last changes fastest.
Arguments:
- conserved: float32 [8, 512, 64, 128], P(None, 'radial', 'phi'), may hold values from -2.5 to 7, as said below
- core_mass: float32 [1], replicated, may hold values from 0.2 to 1
Outputs:
- advanced: float32 [8, 512, 64, 128], P(None, 'radial', 'phi')
- enclosed_mass: float32 [512], P('radial')
The draws below stay inside these ranges and needn't reach their ends.
Inputs may be any that keep to these rules, and one draw needn't show every extreme that they name: conserved[0] (density) lies between 0.4 and 2.5; conserved[4] exceeds (conserved[1]^2 + conserved[2]^2 + conserved[3]^2)/(2 conserved[0]) by at least 0.6; the speeds |conserved[m]/conserved[0]| stay below 1; conserved[5..7] lie between 0 and conserved[0].
All inputs are finite; a program needn't handle non-finite values.
Results may differ from the reference program's by a relative error of at most 0.0003.
Values sent between devices are 32-bit elements; how exact they have to be, the bound alone decides.
No kernel may reach another device: no remote copies, remote signals or barrier semaphores. Data moves between devices by JAX's collectives and lax.ppermute only.
A program may use at most 64 MiB of HBM per device.

```python
import math
import jax
import jax.numpy as jnp
from jax import lax

RD = 8
NT = 128
NR = 512
NP = 64


def draw_conserved(key, part):
    subkeys = jax.random.split(key, 12)
    shape = (NR, NP, NT)
    depth = (jnp.arange(NR, dtype=jnp.float32) + 0.5) / NR
    azimuth = (jnp.arange(NP, dtype=jnp.float32) + 0.5) * (2.0 * math.pi / NP)
    centres = jax.random.uniform(subkeys[6], (3,), jnp.float32, 0.0, 1.0)
    heights = jax.random.uniform(subkeys[7], (3,), jnp.float32, -0.13, 0.13)
    bumps = jnp.exp(-jnp.square((depth[:, None] - centres[None, :]) / 0.15))
    profile = jnp.exp(jnp.sum(bumps * heights[None, :], axis=1))
    turn = jax.random.uniform(subkeys[8], (), jnp.float32, 0.0, 2.0 * math.pi)
    twist = jax.random.uniform(subkeys[9], (), jnp.float32, -0.5 * math.pi, 0.5 * math.pi)
    phase = turn + twist * depth
    angular = 1.0 + 0.35 * jnp.cos(azimuth[None, :] - phase[:, None])
    smooth = (profile[:, None] * angular)[:, :, None]
    rough = jnp.exp(jax.random.uniform(subkeys[0], shape, jnp.float32, jnp.log(0.75), jnp.log(1.33)))
    density = jnp.clip(smooth * rough, 0.4, 2.5)
    speeds = [jnp.clip(0.3 * jax.random.normal(subkeys[1 + which], shape, jnp.float32), -0.99, 0.99) for which in range(3)]
    pressure = jax.random.uniform(subkeys[4], shape, jnp.float32, 0.3, 0.9)
    kinetic = 0.5 * density * (speeds[0] * speeds[0] + speeds[1] * speeds[1] + speeds[2] * speeds[2])
    energy = pressure / (4.0 / 3.0 - 1.0) + kinetic
    tracers = jax.random.uniform(subkeys[5], (3,) + shape, jnp.float32, 0.0, 1.0) * density[None]
    momenta = jnp.stack([density * speeds[0], density * speeds[1], density * speeds[2]])
    return jnp.concatenate([density[None], momenta, energy[None], tracers], axis=0)


def setup_inputs(seed: int = 0) -> dict:
    streams_of = jax.random.split(jax.random.key(seed), 3)
    conserved = draw_conserved(jax.random.fold_in(streams_of[2], 71), 0)
    core_mass = jnp.clip(jnp.exp(jax.random.uniform(streams_of[1], (1,), jnp.float32, math.log(0.2), math.log(1.0))), 0.2, 1.0)
    return {"conserved": conserved, "core_mass": core_mass}


ADIABATIC = 4.0 / 3.0
INNER_RADIUS = 1.0
OUTER_RADIUS = 2.0
COURANT = 0.4
GRAVITY_KICK = 0.004
MINIMUM_DENSITY = 0.05
PRESSURE_FLOOR = 0.01

def step_sizes(radial_total, phi_total, theta_total):
    theta_step = math.pi / theta_total
    phi_step = 2.0 * math.pi / phi_total
    polar_width = INNER_RADIUS * math.sin(0.5 * theta_step) * phi_step
    radial_step = min(2.0 * polar_width, (OUTER_RADIUS - INNER_RADIUS) / radial_total)
    timestep = COURANT * min(radial_step, polar_width)
    return (radial_step, theta_step, phi_step, timestep)

def thermo(values):
    density = jnp.maximum(values[0], MINIMUM_DENSITY)
    kinetic = 0.5 * (values[1] * values[1] + values[2] * values[2] + values[3] * values[3]) / density
    pressure = jnp.maximum((ADIABATIC - 1.0) * (values[4] - kinetic), PRESSURE_FLOOR * density)
    return (density, pressure)

def physical(values, component):
    density, pressure = thermo(values)
    normal = values[component] / density
    sound = jnp.sqrt(ADIABATIC * pressure / density)
    pieces = [values[which] * normal for which in range(values.shape[0])]
    pieces[component] = pieces[component] + pressure
    pieces[4] = pieces[4] + pressure * normal
    return (jnp.stack(pieces), jnp.abs(normal) + sound)

def face_flux(values, along_dim, component):
    interior = values.shape[along_dim] - 4
    neighbour_differences = lax.slice_in_dim(values, 1, interior + 4, axis=along_dim) - lax.slice_in_dim(values, 0, interior + 3, axis=along_dim)
    below_diff = lax.slice_in_dim(neighbour_differences, 0, interior + 2, axis=along_dim)
    above_diff = lax.slice_in_dim(neighbour_differences, 1, interior + 3, axis=along_dim)
    limited = 0.5 * (jnp.sign(below_diff) + jnp.sign(above_diff)) * jnp.minimum(jnp.abs(below_diff), jnp.abs(above_diff))
    left_state = lax.slice_in_dim(values, 1, interior + 2, axis=along_dim) + 0.5 * lax.slice_in_dim(limited, 0, interior + 1, axis=along_dim)
    right_state = lax.slice_in_dim(values, 2, interior + 3, axis=along_dim) - 0.5 * lax.slice_in_dim(limited, 1, interior + 2, axis=along_dim)
    left_flux, left_signal = physical(left_state, component)
    right_flux, right_signal = physical(right_state, component)
    signal = jnp.maximum(left_signal, right_signal)
    return 0.5 * (left_flux + right_flux) - 0.5 * signal * (right_state - left_state)

def hydro_rate(extended, cell_centers, enclosed, radial_step, theta_step, phi_step, strength):
    theta_cells = extended.shape[3]
    centre_cells = extended[:, 2:-2, 2:-2, :]
    polar_padded = jnp.pad(centre_cells, ((0, 0), (0, 0), (0, 0), (2, 2)), mode='edge')
    radial_flux = face_flux(extended[:, :, 2:-2, :], 1, 1)
    polar_flux = face_flux(polar_padded, 3, 2)
    azimuth_flux = face_flux(extended[:, 2:-2, :, :], 2, 3)
    angles = (jnp.arange(theta_cells, dtype=jnp.float32) + 0.5) * theta_step
    sine_center = jnp.sin(angles)
    cosine = jnp.cos(angles)
    face_sine = jnp.sin(jnp.arange(theta_cells + 1, dtype=jnp.float32) * theta_step)
    radius = cell_centers[:, None, None]
    face_radius = jnp.concatenate([cell_centers - 0.5 * radial_step, cell_centers[-1:] + 0.5 * radial_step])[:, None, None]
    radial_area = face_radius * face_radius * radial_flux
    divergence = (radial_area[:, 1:] - radial_area[:, :-1]) / (radius * radius * radial_step)
    polar_area = face_sine * polar_flux
    divergence = divergence + (polar_area[..., 1:] - polar_area[..., :-1]) / (radius * sine_center * theta_step)
    divergence = divergence + (azimuth_flux[:, :, 1:] - azimuth_flux[:, :, :-1]) / (radius * sine_center * phi_step)
    density, pressure = thermo(centre_cells)
    radial_speed = centre_cells[1] / density
    polar_speed = centre_cells[2] / density
    azimuth_speed = centre_cells[3] / density
    cotangent = cosine / sine_center
    gravity_pull = strength * enclosed[:, None, None] / (radius * radius)
    source_radial = (2.0 * pressure + density * (polar_speed * polar_speed + azimuth_speed * azimuth_speed)) / radius - density * gravity_pull
    source_polar = (pressure * cotangent + density * azimuth_speed * azimuth_speed * cotangent - density * radial_speed * polar_speed) / radius
    source_azimuth = -density * azimuth_speed * (radial_speed + polar_speed * cotangent) / radius
    source_energy = -centre_cells[1] * gravity_pull
    nothing = jnp.zeros_like(pressure)
    source = jnp.stack([nothing, source_radial, source_polar, source_azimuth, source_energy, nothing, nothing, nothing])
    return source - divergence

def reference(conserved, core_mass):
    radial_total = conserved.shape[1]
    phi_total = conserved.shape[2]
    theta_total = conserved.shape[3]
    radial_step, theta_step, phi_step, timestep = step_sizes(radial_total, phi_total, theta_total)
    strength = GRAVITY_KICK / timestep
    cell_centers = INNER_RADIUS + (jnp.arange(radial_total, dtype=jnp.float32) + 0.5) * radial_step
    sine_center = jnp.sin((jnp.arange(theta_total, dtype=jnp.float32) + 0.5) * theta_step)
    shells = jnp.dot(lax.optimization_barrier(jnp.sum(conserved[0], axis=1)), sine_center, precision=lax.Precision.HIGHEST)
    shells = shells * cell_centers * cell_centers * (radial_step * theta_step * phi_step)
    enclosed = core_mass[0] + jnp.cumsum(shells) - 0.5 * shells
    blocks = radial_total // RD

    def full_rate(values):
        padded = jnp.pad(values, ((0, 0), (2, 2), (0, 0), (0, 0)), mode='edge')
        padded = jnp.pad(padded, ((0, 0), (0, 0), (2, 2), (0, 0)), mode='wrap')

        def one_block(block_index):
            first_row = (block_index * RD).astype(jnp.int32)
            radial_segment = lax.dynamic_slice_in_dim(padded, first_row, RD + 4, 1)
            radius_part = lax.dynamic_slice_in_dim(cell_centers, first_row, RD, 0)
            mass_part = lax.dynamic_slice_in_dim(enclosed, first_row, RD, 0)
            return hydro_rate(radial_segment, radius_part, mass_part, radial_step, theta_step, phi_step, strength)
        stacked = lax.map(one_block, jnp.arange(blocks, dtype=jnp.int32))
        return jnp.transpose(stacked, (1, 0, 2, 3, 4)).reshape(values.shape)
    section_one = conserved + timestep * full_rate(conserved)
    section_two = section_one + timestep * full_rate(section_one)
    advanced = 0.5 * conserved + 0.5 * section_two
    return (advanced, enclosed)
```

```python
import math

import jax
import jax.numpy as jnp
import numpy as np
from jax import lax
from jax.experimental import pallas as pl
from jax.experimental.pallas import tpu as pltpu
from jax.sharding import PartitionSpec as P

ADIABATIC = 4.0 / 3.0
INNER_RADIUS = 1.0
OUTER_RADIUS = 2.0
COURANT = 0.4
GRAVITY_KICK = 0.004
MINIMUM_DENSITY = 0.05
PRESSURE_FLOOR = 0.01
NV = 8
LANES = 128
VMEM_LIMIT = 12 * 1024 * 1024


def step_sizes(radial_total, phi_total, theta_total):
    theta_step = math.pi / theta_total
    phi_step = 2.0 * math.pi / phi_total
    polar_width = INNER_RADIUS * math.sin(0.5 * theta_step) * phi_step
    radial_step = min(2.0 * polar_width, (OUTER_RADIUS - INNER_RADIUS) / radial_total)
    timestep = COURANT * min(radial_step, polar_width)
    return (radial_step, theta_step, phi_step, timestep)


def angle_table(theta_cells, theta_step, phi_step):
    angles = (np.arange(theta_cells, dtype=np.float32) + np.float32(0.5)) * np.float32(theta_step)
    sine, cosine = np.sin(angles), np.cos(angles)
    faces = np.sin(np.arange(theta_cells + 1, dtype=np.float32) * np.float32(theta_step))
    rows = [sine, cosine / sine, faces[1:], faces[:-1], 1.0 / (sine * theta_step), 1.0 / (sine * phi_step)]
    table = np.zeros((8, theta_cells), np.float32)
    for k, row in enumerate(rows):
        table[k] = row
    return table


def half_slope(below, above):
    return jnp.maximum(jnp.minimum(below, above), 0.0) + jnp.minimum(jnp.maximum(below, above), 0.0)


def thermo(u):
    density = jnp.maximum(u[0], MINIMUM_DENSITY)
    inverse = 1.0 / density
    kinetic = 0.5 * (u[1] * u[1] + u[2] * u[2] + u[3] * u[3]) * inverse
    pressure = jnp.maximum((ADIABATIC - 1.0) * (u[4] - kinetic), PRESSURE_FLOOR * density)
    return density, inverse, pressure


def side(u, component):
    _, inverse, pressure = thermo(u)
    normal = u[component] * inverse
    sound = jnp.sqrt((ADIABATIC * pressure) * inverse)
    return normal, pressure, jnp.abs(normal) + sound


def face_flux(left, right, component):
    vl, pl_, al = side(left, component)
    vr, pr, ar = side(right, component)
    signal = jnp.maximum(al, ar)
    out = []
    for k in range(NV):
        if k == 4:
            total = (left[k] + pl_) * vl + (right[k] + pr) * vr
        else:
            total = left[k] * vl + right[k] * vr
        if k == component:
            total = total + (pl_ + pr)
        out.append(total - signal * (right[k] - left[k]))
    return out


def rate_rows(x, radial_flux, left_row, table, rows, wide, first_row, steps, emit):
    radial_step = steps[0]
    ring = x.shape[2]

    def radius_of(index):
        return INNER_RADIUS + (jnp.full((1, LANES), index, jnp.float32) + 0.5) * radial_step

    def states(j):
        left, right = [], []
        for k in range(NV):
            centre = x[k, j, :wide]
            slope = half_slope(0.5 * (centre - x[k, j - 1, :wide]), 0.5 * (x[k, j + 1, :wide] - centre))
            left.append(centre + slope)
            right.append(centre - slope)
        return left, right

    left, _ = states(1)
    for k in range(NV):
        left_row[k] = left[k]

    def radial_face(f, carry):
        above, right = states(f + 2)
        flux = face_flux([left_row[k] for k in range(NV)], right, 1)
        face = radius_of((first_row + f).astype(jnp.float32)) - 0.5 * radial_step
        area = 0.5 * face * face
        for k in range(NV):
            radial_flux[f, k] = area * flux[k]
            left_row[k] = above[k]
        return carry

    lax.fori_loop(0, rows + 1, radial_face, 0)

    last = lax.broadcasted_iota(jnp.int32, (wide, LANES), 1) == LANES - 1

    def row(r, carry):
        radius = radius_of((first_row + r).astype(jnp.float32))
        inverse_radius = 1.0 / radius
        radial_scale = inverse_radius * inverse_radius * (1.0 / radial_step)
        u = [x[k, r + 2, :wide] for k in range(NV)]
        rate = []
        for k in range(NV):
            rate.append((radial_flux[r, k] - radial_flux[r + 1, k]) * radial_scale)
        left, right = [], []
        for k in range(NV):
            above = jnp.where(last, 0.0, 0.5 * (pltpu.roll(u[k], LANES - 1, 1) - u[k]))
            below = pltpu.roll(above, 1, 1)
            slope = half_slope(below, above)
            left.append(u[k] + slope)
            right.append(jnp.where(last, u[k], pltpu.roll(u[k] - slope, LANES - 1, 1)))
        flux = face_flux(left, right, 2)
        polar_scale = table[4:5, :] * (0.5 * inverse_radius)
        upper, lower = table[2:3, :] * polar_scale, table[3:4, :] * polar_scale
        for k in range(NV):
            rate[k] = rate[k] - (upper * flux[k] - lower * pltpu.roll(flux[k], 1, 1))
        left, right = [], []
        for k in range(NV):
            ext = x[k, r + 2]
            above = 0.5 * (pltpu.roll(ext, ring - 1, 0) - ext)
            below = pltpu.roll(above, 1, 0)
            slope = half_slope(below, above)
            left.append(ext + slope)
            right.append(pltpu.roll(ext - slope, ring - 1, 0))
        flux = face_flux(left, right, 3)
        azimuth_scale = table[5:6, :] * (0.5 * inverse_radius)
        for k in range(NV):
            rate[k] = rate[k] - azimuth_scale * (flux[k][:wide] - pltpu.roll(flux[k], 1, 0)[:wide])
        density, inverse, pressure = thermo(u)
        cotangent = table[1:2, :]
        vr, vt, vp = u[1] * inverse, u[2] * inverse, u[3] * inverse
        azimuth_push = density * vp * vp
        rate[1] = rate[1] + (2.0 * pressure + (density * vt * vt + azimuth_push)) * inverse_radius
        rate[2] = rate[2] + ((pressure + azimuth_push) * cotangent - density * vr * vt) * inverse_radius
        rate[3] = rate[3] - density * vp * (vr + vt * cotangent) * inverse_radius
        emit(r, u, rate)
        return carry

    lax.fori_loop(0, rows, row, 0)


def fill_ends(x, rows, position, last_position):
    first = (x.shape[1] - rows) // 2
    last = first + rows - 1

    @pl.when(position == 0)
    def _():
        for k in range(NV):
            x[k, first - 2] = x[k, first]
            x[k, first - 1] = x[k, first]

    @pl.when(position == last_position)
    def _():
        for k in range(NV):
            x[k, last + 1] = x[k, last]
            x[k, last + 2] = x[k, last]


def solution(mesh):
    radial_devices, phi_devices = mesh.shape["radial"], mesh.shape["phi"]
    assert phi_devices == 4
    up = [(i, (i + 1) % radial_devices) for i in range(radial_devices)]
    down = [(j, i) for i, j in up]
    clockwise = [(i, (i + 1) % phi_devices) for i in range(phi_devices)]
    counter = [(j, i) for i, j in clockwise]
    opposite = [(i, (i + 2) % phi_devices) for i in range(phi_devices)]

    def body(conserved, core_mass):
        _, rows, wedge, theta_cells = conserved.shape
        steps = step_sizes(rows * radial_devices, wedge * phi_devices, theta_cells)
        radial_step, theta_step, phi_step, timestep = steps
        strength = GRAVITY_KICK / timestep
        ring, outer = wedge + 8, rows + 4
        table = jnp.asarray(angle_table(theta_cells, theta_step, phi_step))
        position = lax.axis_index("radial").astype(jnp.int32).reshape(1)
        smem = pl.BlockSpec(memory_space=pltpu.SMEM)
        vmem = pl.BlockSpec(memory_space=pltpu.VMEM)
        f32 = jnp.float32
        limit = pltpu.CompilerParams(vmem_limit_bytes=VMEM_LIMIT)

        def shape(*sizes):
            return jax.ShapeDtypeStruct(sizes, f32)

        def radius_at(index):
            return INNER_RADIUS + (jnp.full((1, LANES), index, f32) + 0.5) * radial_step

        side_rows = NV * rows * 4

        def pack(where, u, angles, mass, before, after):
            lane = lax.broadcasted_iota(jnp.int32, (1, LANES), 1)
            line = jnp.zeros((1, LANES), f32)
            for r in range(rows):
                radius = radius_at((where[0] * rows + r).astype(f32))
                total = jnp.sum(u[0, r] * angles[0:1, :], axis=(0, 1), keepdims=True)
                shell = total * (radius * radius * (radial_step * theta_step * phi_step))
                line = jnp.where(lane == r, shell, line)
            tile = jnp.broadcast_to(line, (8, LANES))
            mass[...] = tile
            for target, start in ((before, 0), (after, wedge - 4)):
                target[side_rows : side_rows + 8] = tile
                for k in range(NV):
                    for r in range(rows):
                        at = (k * rows + r) * 4
                        target[at : at + 4] = u[k, r, start : start + 4]

        mass, wedge_before, wedge_after = pl.pallas_call(
            pack,
            out_shape=[shape(8, LANES), shape(side_rows + 8, LANES), shape(side_rows + 8, LANES)],
            in_specs=[smem, vmem, vmem],
            out_specs=[vmem] * 3,
            compiler_params=limit,
            name="pack",
        )(position, conserved, table)

        wedge_low = lax.ppermute(wedge_after, "phi", clockwise)
        wedge_high = lax.ppermute(wedge_before, "phi", counter)
        mass_across = lax.ppermute(mass, "phi", opposite)

        def sides(u, low, high, own, across, h, before, after, masses):
            for k in range(NV):
                for r in range(rows):
                    at = (k * rows + r) * 4
                    h[k, r, 0:4] = high[at : at + 4]
                    h[k, r, 4:8] = low[at : at + 4]
                for r in range(4):
                    before[k, r * wedge : (r + 1) * wedge] = u[k, r]
                    after[k, r * wedge : (r + 1) * wedge] = u[k, rows - 4 + r]
                for r in range(2):
                    at = 4 * wedge + 8 * r
                    before[k, at : at + 8] = h[k, r]
                    after[k, at : at + 8] = h[k, rows - 2 + r]
            beside = low[side_rows : side_rows + 8] + high[side_rows : side_rows + 8]
            total = (own[...] + across[...]) + beside
            masses[...] = jnp.concatenate([total] * (radial_devices // 8), axis=0)

        edge = shape(NV, 4 * wedge + 16, LANES)
        h, before, after, masses = pl.pallas_call(
            sides,
            out_shape=[shape(NV, rows, 8, LANES), edge, edge, shape(radial_devices, LANES)],
            in_specs=[vmem] * 5,
            out_specs=[vmem] * 4,
            compiler_params=limit,
            name="sides",
        )(conserved, wedge_low, wedge_high, mass, mass_across)

        low = lax.ppermute(after, "radial", up)
        high = lax.ppermute(before, "radial", down)
        everyone = lax.all_to_all(masses, "radial", 0, 0, tiled=True)

        def first_section(where, u, h, low, high, angles, out, pulled, x, radial_flux, left_row):
            ones = jnp.ones((8, LANES), f32)
            for k in range(NV):
                for r in range(4):
                    x[k, r, 0:wedge] = low[k, r * wedge : (r + 1) * wedge]
                    x[k, rows + 4 + r, 0:wedge] = high[k, r * wedge : (r + 1) * wedge]
                for r in range(2):
                    at = 4 * wedge + 8 * r
                    x[k, r, wedge:ring] = ones
                    x[k, r + 2, wedge:ring] = low[k, at : at + 8]
                    x[k, rows + 4 + r, wedge:ring] = high[k, at : at + 8]
                    x[k, rows + 6 + r, wedge:ring] = ones
                for r in range(rows):
                    x[k, r + 4, 0:wedge] = u[k, r]
                    x[k, r + 4, wedge:ring] = h[k, r]
            fill_ends(x, rows, where[0], radial_devices - 1)

            def emit(r, state, rate):
                for k in range(NV):
                    out[k, r] = state[k] + timestep * rate[k]
                pulled[0, r] = jnp.maximum(state[0], MINIMUM_DENSITY)
                pulled[1, r] = state[1]

            rate_rows(x, radial_flux, left_row, angles, outer, ring, where[0] * rows - 2, steps, emit)

        partial, pulled = pl.pallas_call(
            first_section,
            out_shape=[shape(NV, outer, ring, LANES), shape(2, outer, ring, LANES)],
            in_specs=[smem] + [vmem] * 5,
            out_specs=[vmem] * 2,
            scratch_shapes=[
                pltpu.VMEM((NV, rows + 8, ring, LANES), f32),
                pltpu.VMEM((outer + 1, NV, ring, LANES), f32),
                pltpu.VMEM((NV, ring, LANES), f32),
            ],
            compiler_params=limit,
            name="first_section",
        )(position, conserved, h, low, high, table)

        def second_section(where, core, masses, u, part, pulled, angles, out, enclosed, x, radial_flux, left_row, pulls):
            first = where[0] * rows
            device = lax.broadcasted_iota(jnp.int32, (radial_devices, LANES), 0)
            lane = lax.broadcasted_iota(jnp.int32, (radial_devices, LANES), 1)
            zone = device * rows + lane
            shell = jnp.where(lane < rows, masses[...], 0.0)
            line = jnp.zeros((1, LANES), f32)
            for j in range(outer):
                index = first + (j - 2)
                weight = jnp.where(zone < index, 1.0, jnp.where(zone == index, 0.5, 0.0))
                inside = jnp.sum(shell * weight, axis=(0, 1), keepdims=True) + core[0]
                radius = radius_at(index.astype(f32))
                pull = (timestep * strength) * inside / (radius * radius)
                pulls[j] = pull
                line = jnp.where(lane[0:1] == j - 2, inside, line)
                for k in range(NV):
                    if k == 1:
                        x[k, j] = part[k, j] - pull * pulled[0, j]
                    elif k == 4:
                        x[k, j] = part[k, j] - pull * pulled[1, j]
                    else:
                        x[k, j] = part[k, j]
            enclosed[...] = line
            fill_ends(x, rows, where[0], radial_devices - 1)

            def emit(r, state, rate):
                pull = pulls[r + 2]
                density = jnp.maximum(state[0], MINIMUM_DENSITY)
                for k in range(NV):
                    change = timestep * rate[k]
                    if k == 1:
                        change = change - pull * density
                    if k == 4:
                        change = change - pull * state[1]
                    out[k, r] = 0.5 * u[k, r] + 0.5 * (state[k] + change)

            rate_rows(x, radial_flux, left_row, angles, rows, wedge, first, steps, emit)

        advanced, enclosed = pl.pallas_call(
            second_section,
            out_shape=[shape(*conserved.shape), shape(1, LANES)],
            in_specs=[smem, smem] + [vmem] * 5,
            out_specs=[vmem] * 2,
            scratch_shapes=[
                pltpu.VMEM((NV, outer, ring, LANES), f32),
                pltpu.VMEM((rows + 1, NV, wedge, LANES), f32),
                pltpu.VMEM((NV, wedge, LANES), f32),
                pltpu.VMEM((outer, 1, LANES), f32),
            ],
            compiler_params=limit,
            name="second_section",
        )(position, core_mass, everyone, conserved, partial, pulled, table)
        return advanced, enclosed[0, :rows]

    in_specs = (P(None, "radial", "phi", None), P())
    out_specs = (P(None, "radial", "phi", None), P("radial"))
    return jax.shard_map(body, mesh=mesh, in_specs=in_specs, out_specs=out_specs, check_vma=False)
```

```python
import math

import jax
import jax.numpy as jnp
from jax import lax
from jax.experimental import pallas as pl
from jax.experimental.pallas import tpu as pltpu
from jax.sharding import PartitionSpec as P

ADIABATIC = 4.0 / 3.0
INNER_RADIUS = 1.0
OUTER_RADIUS = 2.0
COURANT = 0.4
GRAVITY_KICK = 0.004
MINIMUM_DENSITY = 0.05
PRESSURE_FLOOR = 0.01
NV = 8
LANES = 128
SUBLANES = 8
UNROLL1 = 2
UNROLL2 = 4
VMEM_LIMIT = 12 * 1024 * 1024


def step_sizes(radial_total, phi_total, theta_total):
    theta_step = math.pi / theta_total
    phi_step = 2.0 * math.pi / phi_total
    polar_width = INNER_RADIUS * math.sin(0.5 * theta_step) * phi_step
    radial_step = min(2.0 * polar_width, (OUTER_RADIUS - INNER_RADIUS) / radial_total)
    timestep = COURANT * min(radial_step, polar_width)
    return (radial_step, theta_step, phi_step, timestep)


def splat(value):
    return jnp.full((SUBLANES, LANES), value, jnp.float32)


def lane_index():
    return lax.broadcasted_iota(jnp.int32, (SUBLANES, LANES), 1)


def sine_of_zones(theta_step):
    return jnp.sin((lane_index().astype(jnp.float32) + 0.5) * theta_step)


def fill_angles(angles, steps):
    _, theta_step, phi_step, _ = steps
    lane = lane_index().astype(jnp.float32)
    sine = sine_of_zones(theta_step)
    angles[0] = jnp.cos((lane + 0.5) * theta_step) / sine
    angles[1] = jnp.sin((lane + 1.0) * theta_step) * (0.5 / (sine * theta_step))
    angles[2] = jnp.sin(lane * theta_step) * (0.5 / (sine * theta_step))
    angles[3] = 0.5 / (sine * phi_step)


def half_slope(below, above):
    return 0.5 * jnp.maximum(jnp.minimum(above, jnp.maximum(below, 0.0)), jnp.minimum(below, 0.0))


def thermo(u):
    density = jnp.maximum(u[0], MINIMUM_DENSITY)
    inverse = 1.0 / density
    kinetic = (0.5 * inverse) * (u[1] * u[1] + u[2] * u[2] + u[3] * u[3])
    pressure = jnp.maximum((ADIABATIC - 1.0) * (u[4] - kinetic), PRESSURE_FLOOR * density)
    return density, inverse, pressure


def side(u, component):
    _, inverse, pressure = thermo(u)
    normal = u[component] * inverse
    square = (ADIABATIC * pressure) * inverse
    return normal, pressure, jnp.abs(normal) + square * lax.rsqrt(square)


def face_flux(left, right, component):
    vl, pl_, al = side(left, component)
    vr, pr, ar = side(right, component)
    signal = jnp.maximum(al, ar)
    toward, away = vl + signal, vr - signal
    out = [left[k] * toward + right[k] * away for k in range(NV)]
    out[component] = out[component] + (pl_ + pr)
    out[4] = out[4] + (pl_ * vl + pr * vr)
    return out


def next_zone(value, edge):
    turned = pltpu.roll(value, SUBLANES - 1, 1)
    return jnp.where(edge, jnp.concatenate([turned[1:], turned[:1]], axis=0), turned)


def previous_zone(value, edge):
    turned = pltpu.roll(value, 1, 1)
    return jnp.where(edge, jnp.concatenate([turned[-1:], turned[:-1]], axis=0), turned)


def rate_rows(x, kept, angles, rows, wide, first_row, steps, unroll, emit):
    radial_step = steps[0]

    def radius_of(index):
        return INNER_RADIUS + (splat(index) + 0.5) * radial_step

    def states(j, below):
        left, right, above = [], [], []
        for k in range(NV):
            centre = x[j, k, :wide]
            difference = x[j + 1, k, :wide] - centre
            slope = half_slope(below[k], difference)
            left.append(centre + slope)
            right.append(centre - slope)
            above.append(difference)
        return left, right, above

    def keep(left, above):
        for k in range(NV):
            kept[0, k] = left[k]
            kept[1, k] = above[k]

    def radial_face(f):
        inner = [kept[0, k] for k in range(NV)]
        left, right, above = states(f + 2, [kept[1, k] for k in range(NV)])
        keep(left, above)
        face = radius_of(jnp.asarray(first_row + f).astype(jnp.float32)) - 0.5 * radial_step
        area = (0.5 / radial_step) * face * face
        return [area * value for value in face_flux(inner, right, 1)]

    left, _, above = states(1, [x[1, k, :wide] - x[0, k, :wide] for k in range(NV)])
    keep(left, above)
    for k, value in enumerate(radial_face(0)):
        kept[2, k] = value

    last = lane_index() == LANES - 1
    sublane = lax.broadcasted_iota(jnp.int32, (SUBLANES, LANES), 0)
    top, bottom = sublane == SUBLANES - 1, sublane == 0

    def row(r, carry):
        inverse_radius = 1.0 / radius_of((first_row + r).astype(jnp.float32))
        radial_scale = inverse_radius * inverse_radius
        u = [x[r + 2, k, :wide] for k in range(NV)]
        upper = radial_face(r + 1)
        rate = [(kept[2, k] - upper[k]) * radial_scale for k in range(NV)]
        for k in range(NV):
            kept[2, k] = upper[k]
        left, right = [], []
        for k in range(NV):
            after = jnp.where(last, u[k], pltpu.roll(u[k], LANES - 1, 2))
            above = after - u[k]
            slope = half_slope(pltpu.roll(above, 1, 2), above)
            left.append(u[k] + slope)
            right.append(after - pltpu.roll(slope, LANES - 1, 2))
        flux = face_flux(left, right, 2)
        upper, lower = angles[1] * inverse_radius, angles[2] * inverse_radius
        for k in range(NV):
            rate[k] = rate[k] - (upper * flux[k] - lower * pltpu.roll(flux[k], 1, 2))
        left, right = [], []
        for k in range(NV):
            zones = x[r + 2, k]
            after = next_zone(zones, top)
            above = after - zones
            slope = half_slope(previous_zone(above, bottom), above)
            left.append(zones + slope)
            right.append(after - next_zone(slope, top))
        flux = face_flux(left, right, 3)
        scale = angles[3] * inverse_radius
        for k in range(NV):
            rate[k] = rate[k] - scale * (flux[k][:wide] - previous_zone(flux[k], bottom)[:wide])
        density, inverse, pressure = thermo(u)
        cotangent = angles[0]
        vr, vt, vp = u[1] * inverse, u[2] * inverse, u[3] * inverse
        azimuth_push = density * vp * vp
        polar_carry = density * vt
        rate[1] = rate[1] + (2.0 * pressure + (polar_carry * vt + azimuth_push)) * inverse_radius
        rate[2] = rate[2] + ((pressure + azimuth_push) * cotangent - polar_carry * vr) * inverse_radius
        rate[3] = rate[3] - density * vp * (vr + vt * cotangent) * inverse_radius
        emit(r, u, rate)
        return carry

    lax.fori_loop(0, rows, row, 0, unroll=unroll)


def fill_ends(x, rows, position, last_position):
    first = (x.shape[0] - rows) // 2
    last = first + rows - 1

    @pl.when(position == 0)
    def _():
        for k in range(NV):
            x[first - 2, k] = x[first, k]
            x[first - 1, k] = x[first, k]

    @pl.when(position == last_position)
    def _():
        for k in range(NV):
            x[last + 1, k] = x[last, k]
            x[last + 2, k] = x[last, k]


def solution(mesh):
    radial_devices, phi_devices = mesh.shape["radial"], mesh.shape["phi"]
    assert phi_devices == 4
    up = [(i, (i + 1) % radial_devices) for i in range(radial_devices)]
    down = [(j, i) for i, j in up]
    clockwise = [(i, (i + 1) % phi_devices) for i in range(phi_devices)]
    counter = [(j, i) for i, j in clockwise]
    opposite = [(i, (i + 2) % phi_devices) for i in range(phi_devices)]

    def body(conserved, core_mass):
        _, rows, wedge, theta_cells = conserved.shape
        steps = step_sizes(rows * radial_devices, wedge * phi_devices, theta_cells)
        radial_step, theta_step, phi_step, timestep = steps
        strength = GRAVITY_KICK / timestep
        own = wedge // SUBLANES
        tiles, outer = own + 1, rows + 4
        zones = conserved.reshape(NV, rows, own, SUBLANES, theta_cells)
        position = lax.axis_index("radial").astype(jnp.int32).reshape(1)
        smem = pl.BlockSpec(memory_space=pltpu.SMEM)
        vmem = pl.BlockSpec(memory_space=pltpu.VMEM)
        hbm = pl.BlockSpec(memory_space=pl.ANY)
        f32 = jnp.float32
        limit = pltpu.CompilerParams(vmem_limit_bytes=VMEM_LIMIT)
        angle_scratch = pltpu.VMEM((4, SUBLANES, LANES), f32)

        def shape(*sizes):
            return jax.ShapeDtypeStruct(sizes, f32)

        def radius_at(index):
            return INNER_RADIUS + (splat(index) + 0.5) * radial_step

        def whole(value):
            return jnp.sum(value, axis=(0, 1), keepdims=True)

        side_rows = NV * rows * 4
        corner = 4 * own

        def pack(where, u, mass, wedge_before, wedge_after, before, after):
            sine = sine_of_zones(theta_step)
            lane = lane_index()
            tile = jnp.zeros((SUBLANES, LANES), f32)
            for r in range(rows):
                radius = radius_at((where[0] * rows + r).astype(f32))
                total = sum(u[0, r, t] for t in range(1, own)) + u[0, r, 0]
                shell = whole(total * sine) * (radius * radius * (radial_step * theta_step * phi_step))
                tile = jnp.where(lane == r, shell, tile)
            mass[...] = tile
            wedge_before[side_rows : side_rows + 8] = tile
            wedge_after[side_rows : side_rows + 8] = tile
            for k in range(NV):
                for r in range(rows):
                    at = (k * rows + r) * 4
                    wedge_before[at : at + 4] = u[k, r, 0, 0:4]
                    wedge_after[at : at + 4] = u[k, r, own - 1, 4:8]
                for r in range(4):
                    for t in range(own):
                        before[k, r * own + t] = u[k, r, t]
                        after[k, r * own + t] = u[k, rows - 4 + r, t]

        edge = shape(NV, corner + 2, SUBLANES, LANES)
        mass, wedge_before, wedge_after, before, after = pl.pallas_call(
            pack,
            out_shape=[shape(8, LANES), shape(side_rows + 8, LANES), shape(side_rows + 8, LANES), edge, edge],
            in_specs=[smem, vmem],
            out_specs=[vmem] * 5,
            compiler_params=limit,
            name="pack",
        )(position, zones)

        wedge_low = lax.ppermute(wedge_after, "phi", clockwise)
        wedge_high = lax.ppermute(wedge_before, "phi", counter)
        mass_across = lax.ppermute(mass, "phi", opposite)

        def sides(low, high, mass, across, _before, _after, h, before, after, masses):
            for k in range(NV):
                for r in range(rows):
                    at = (k * rows + r) * 4
                    h[k, r, 0:4] = high[at : at + 4]
                    h[k, r, 4:8] = low[at : at + 4]
                for r in range(2):
                    before[k, corner + r] = h[k, r]
                    after[k, corner + r] = h[k, rows - 2 + r]
            beside = low[side_rows : side_rows + 8] + high[side_rows : side_rows + 8]
            total = (mass[...] + across[...]) + beside
            masses[...] = jnp.concatenate([total] * (radial_devices // 8), axis=0)

        h, before, after, masses = pl.pallas_call(
            sides,
            out_shape=[shape(NV, rows, SUBLANES, LANES), edge, edge, shape(radial_devices, LANES)],
            in_specs=[vmem] * 6,
            out_specs=[vmem] * 4,
            input_output_aliases={4: 1, 5: 2},
            compiler_params=limit,
            name="sides",
        )(wedge_low, wedge_high, mass, mass_across, before, after)

        low = lax.ppermute(after, "radial", up)
        high = lax.ppermute(before, "radial", down)
        everyone = lax.all_to_all(masses, "radial", 0, 0, tiled=True)

        def first_section(where, u, h, low, high, out, pulled, x, kept, angles):
            fill_angles(angles, steps)
            ones = splat(1.0)
            for k in range(NV):
                for r in range(4):
                    for t in range(own):
                        x[r, k, t] = low[k, r * own + t]
                        x[rows + 4 + r, k, t] = high[k, r * own + t]
                for r in range(2):
                    x[r, k, own] = ones
                    x[r + 2, k, own] = low[k, corner + r]
                    x[rows + 4 + r, k, own] = high[k, corner + r]
                    x[rows + 6 + r, k, own] = ones
                for r in range(rows):
                    for t in range(own):
                        x[r + 4, k, t] = u[k, r, t]
                    x[r + 4, k, own] = h[k, r]
            fill_ends(x, rows, where[0], radial_devices - 1)

            def emit(r, state, rate):
                for k in range(NV):
                    out[r, k] = state[k] + timestep * rate[k]
                pulled[r, 0] = jnp.maximum(state[0], MINIMUM_DENSITY)
                pulled[r, 1] = state[1]

            rate_rows(x, kept, angles, outer, tiles, where[0] * rows - 2, steps, UNROLL1, emit)

        partial, pulled = pl.pallas_call(
            first_section,
            out_shape=[shape(outer, NV, tiles, SUBLANES, LANES), shape(outer, 2, tiles, SUBLANES, LANES)],
            in_specs=[smem] + [vmem] * 4,
            out_specs=[vmem] * 2,
            scratch_shapes=[
                pltpu.VMEM((rows + 8, NV, tiles, SUBLANES, LANES), f32),
                pltpu.VMEM((3, NV, tiles, SUBLANES, LANES), f32),
                angle_scratch,
            ],
            compiler_params=limit,
            name="first_section",
        )(position, zones, h, low, high)

        def second_section(
            where, core, masses, u, part, pulled, out, enclosed,
            x, kept, angles, pulls, done, sent,
        ):
            fill_angles(angles, steps)
            first = where[0] * rows
            device = lax.broadcasted_iota(jnp.int32, (radial_devices, LANES), 0)
            lane = lax.broadcasted_iota(jnp.int32, (radial_devices, LANES), 1)
            zone = device * rows + lane
            shell = jnp.where(lane < rows, masses[...], 0.0)
            line = jnp.zeros((1, LANES), f32)
            for j in range(outer):
                index = first + (j - 2)
                weight = jnp.where(zone < index, 1.0, jnp.where(zone == index, 0.5, 0.0))
                inside = whole(shell * weight) + core[0]
                radius = radius_at(index.astype(f32))
                pull = (timestep * strength) * inside / (radius * radius)
                pulls[j] = pull
                line = jnp.where(lane[0:1] == j - 2, inside, line)
                for k in range(NV):
                    if k == 1:
                        x[j, k] = part[j, k] - pull * pulled[j, 0]
                    elif k == 4:
                        x[j, k] = part[j, k] - pull * pulled[j, 1]
                    else:
                        x[j, k] = part[j, k]
            enclosed[...] = line[:, :rows]
            fill_ends(x, rows, where[0], radial_devices - 1)

            def leave(r):
                return pltpu.make_async_copy(done.at[r], out.at[:, r], sent.at[r])

            def emit(r, state, rate):
                pull = pulls[r + 2]
                density = jnp.maximum(state[0], MINIMUM_DENSITY)
                for k in range(NV):
                    change = timestep * rate[k]
                    if k == 1:
                        change = change - pull * density
                    if k == 4:
                        change = change - pull * state[1]
                    done[r, k] = 0.5 * u[k, r] + 0.5 * (state[k] + change)
                leave(r).start()

            rate_rows(x, kept, angles, rows, own, first, steps, UNROLL2, emit)
            for r in range(rows):
                leave(r).wait()

        advanced, enclosed = pl.pallas_call(
            second_section,
            out_shape=[shape(*zones.shape), shape(1, rows)],
            in_specs=[smem, smem] + [vmem] * 4,
            out_specs=[hbm, vmem],
            scratch_shapes=[
                pltpu.VMEM((outer, NV, tiles, SUBLANES, LANES), f32),
                pltpu.VMEM((3, NV, own, SUBLANES, LANES), f32),
                angle_scratch,
                pltpu.VMEM((outer, SUBLANES, LANES), f32),
                pltpu.VMEM((rows, NV, own, SUBLANES, LANES), f32),
                pltpu.SemaphoreType.DMA((rows,)),
            ],
            compiler_params=limit,
            name="second_section",
        )(position, core_mass, everyone, zones, partial, pulled)
        return advanced.reshape(conserved.shape), enclosed.reshape(rows)

    in_specs = (P(None, "radial", "phi", None), P())
    out_specs = (P(None, "radial", "phi", None), P("radial"))
    return jax.shard_map(body, mesh=mesh, in_specs=in_specs, out_specs=out_specs, check_vma=False)
```

```python
import math

import jax
import jax.numpy as jnp
from jax import lax
from jax.experimental import pallas as pl
from jax.experimental.pallas import tpu as pltpu
from jax.sharding import PartitionSpec as P

ADIABATIC = 4.0 / 3.0
INNER_RADIUS = 1.0
OUTER_RADIUS = 2.0
COURANT = 0.4
GRAVITY_KICK = 0.004
MINIMUM_DENSITY = 0.05
PRESSURE_FLOOR = 0.01
NV = 8
LANES = 128
SUBLANES = 8
UNROLL1 = 2
UNROLL2 = 4
VMEM_LIMIT = 12 * 1024 * 1024


def step_sizes(radial_total, phi_total, theta_total):
    theta_step = math.pi / theta_total
    phi_step = 2.0 * math.pi / phi_total
    polar_width = INNER_RADIUS * math.sin(0.5 * theta_step) * phi_step
    radial_step = min(2.0 * polar_width, (OUTER_RADIUS - INNER_RADIUS) / radial_total)
    timestep = COURANT * min(radial_step, polar_width)
    return (radial_step, theta_step, phi_step, timestep)


def splat(value):
    return jnp.full((SUBLANES, LANES), value, jnp.float32)


def lane_index():
    return lax.broadcasted_iota(jnp.int32, (SUBLANES, LANES), 1)


def sine_of_zones(theta_step):
    return jnp.sin((lane_index().astype(jnp.float32) + 0.5) * theta_step)


def fill_angles(angles, steps):
    _, theta_step, phi_step, _ = steps
    lane = lane_index().astype(jnp.float32)
    sine = sine_of_zones(theta_step)
    angles[0] = jnp.cos((lane + 0.5) * theta_step) / sine
    angles[1] = jnp.sin((lane + 1.0) * theta_step) * (0.5 / (sine * theta_step))
    angles[2] = jnp.sin(lane * theta_step) * (0.5 / (sine * theta_step))
    angles[3] = 0.5 / (sine * phi_step)


def half_slope(below, above):
    return 0.5 * jnp.maximum(jnp.minimum(above, jnp.maximum(below, 0.0)), jnp.minimum(below, 0.0))


def thermo(u):
    density = jnp.maximum(u[0], MINIMUM_DENSITY)
    inverse = 1.0 / density
    kinetic = (0.5 * inverse) * (u[1] * u[1] + u[2] * u[2] + u[3] * u[3])
    pressure = jnp.maximum((ADIABATIC - 1.0) * (u[4] - kinetic), PRESSURE_FLOOR * density)
    return density, inverse, pressure


def side(u, component):
    _, inverse, pressure = thermo(u)
    normal = u[component] * inverse
    square = (ADIABATIC * pressure) * inverse
    return normal, pressure, jnp.abs(normal) + square * lax.rsqrt(square)


def face_flux(left, right, component):
    vl, pl_, al = side(left, component)
    vr, pr, ar = side(right, component)
    signal = jnp.maximum(al, ar)
    toward, away = vl + signal, vr - signal
    out = [left[k] * toward + right[k] * away for k in range(NV)]
    out[component] = out[component] + (pl_ + pr)
    out[4] = out[4] + (pl_ * vl + pr * vr)
    return out


def next_zone(value, edge):
    turned = pltpu.roll(value, SUBLANES - 1, 1)
    return jnp.where(edge, jnp.concatenate([turned[1:], turned[:1]], axis=0), turned)


def previous_zone(value, edge):
    turned = pltpu.roll(value, 1, 1)
    return jnp.where(edge, jnp.concatenate([turned[-1:], turned[:-1]], axis=0), turned)


def rate_rows(x, kept, angles, rows, wide, first_row, steps, unroll, emit):
    radial_step = steps[0]

    def radius_of(index):
        return INNER_RADIUS + (splat(index) + 0.5) * radial_step

    def states(j, below):
        left, right, above = [], [], []
        for k in range(NV):
            centre = x[j, k, :wide]
            difference = x[j + 1, k, :wide] - centre
            slope = half_slope(below[k], difference)
            left.append(centre + slope)
            right.append(centre - slope)
            above.append(difference)
        return left, right, above

    def keep(left, above):
        for k in range(NV):
            kept[0, k] = left[k]
            kept[1, k] = above[k]

    def radial_face(f):
        inner = [kept[0, k] for k in range(NV)]
        left, right, above = states(f + 2, [kept[1, k] for k in range(NV)])
        keep(left, above)
        face = radius_of(jnp.asarray(first_row + f).astype(jnp.float32)) - 0.5 * radial_step
        area = (0.5 / radial_step) * face * face
        return [area * value for value in face_flux(inner, right, 1)]

    left, _, above = states(1, [x[1, k, :wide] - x[0, k, :wide] for k in range(NV)])
    keep(left, above)
    for k, value in enumerate(radial_face(0)):
        kept[2, k] = value

    last = lane_index() == LANES - 1
    sublane = lax.broadcasted_iota(jnp.int32, (SUBLANES, LANES), 0)
    top, bottom = sublane == SUBLANES - 1, sublane == 0

    def row(r, carry):
        inverse_radius = 1.0 / radius_of((first_row + r).astype(jnp.float32))
        radial_scale = inverse_radius * inverse_radius
        u = [x[r + 2, k, :wide] for k in range(NV)]
        upper = radial_face(r + 1)
        rate = [(kept[2, k] - upper[k]) * radial_scale for k in range(NV)]
        for k in range(NV):
            kept[2, k] = upper[k]
        left, right = [], []
        for k in range(NV):
            after = jnp.where(last, u[k], pltpu.roll(u[k], LANES - 1, 2))
            above = after - u[k]
            slope = half_slope(pltpu.roll(above, 1, 2), above)
            left.append(u[k] + slope)
            right.append(after - pltpu.roll(slope, LANES - 1, 2))
        flux = face_flux(left, right, 2)
        upper, lower = angles[1] * inverse_radius, angles[2] * inverse_radius
        for k in range(NV):
            rate[k] = rate[k] - (upper * flux[k] - lower * pltpu.roll(flux[k], 1, 2))
        left, right = [], []
        for k in range(NV):
            zones = x[r + 2, k]
            after = next_zone(zones, top)
            above = after - zones
            slope = half_slope(previous_zone(above, bottom), above)
            left.append(zones + slope)
            right.append(after - next_zone(slope, top))
        flux = face_flux(left, right, 3)
        scale = angles[3] * inverse_radius
        for k in range(NV):
            rate[k] = rate[k] - scale * (flux[k][:wide] - previous_zone(flux[k], bottom)[:wide])
        density, inverse, pressure = thermo(u)
        cotangent = angles[0]
        vr, vt, vp = u[1] * inverse, u[2] * inverse, u[3] * inverse
        azimuth_push = density * vp * vp
        polar_carry = density * vt
        rate[1] = rate[1] + (2.0 * pressure + (polar_carry * vt + azimuth_push)) * inverse_radius
        rate[2] = rate[2] + ((pressure + azimuth_push) * cotangent - polar_carry * vr) * inverse_radius
        rate[3] = rate[3] - density * vp * (vr + vt * cotangent) * inverse_radius
        emit(r, u, rate)
        return carry

    lax.fori_loop(0, rows, row, 0, unroll=unroll)


def fill_ends(x, rows, position, last_position):
    first = (x.shape[0] - rows) // 2
    last = first + rows - 1

    @pl.when(position == 0)
    def _():
        for k in range(NV):
            x[first - 2, k] = x[first, k]
            x[first - 1, k] = x[first, k]

    @pl.when(position == last_position)
    def _():
        for k in range(NV):
            x[last + 1, k] = x[last, k]
            x[last + 2, k] = x[last, k]


def solution(mesh):
    radial_devices, phi_devices = mesh.shape["radial"], mesh.shape["phi"]
    assert phi_devices == 4 and radial_devices % 2 == 0
    chip = [(i, i ^ 1) for i in range(radial_devices)]
    link = [(i, min(max(i + (1 if i % 2 else -1), 0), radial_devices - 1)) for i in range(radial_devices)]
    clockwise = [(i, (i + 1) % phi_devices) for i in range(phi_devices)]
    counter = [(j, i) for i, j in clockwise]
    pair = [(0, 1), (1, 0), (2, 3), (3, 2)]
    pair_across = [(0, 3), (3, 0), (1, 2), (2, 1)]

    def step(conserved, core_mass):
        _, rows, wedge, theta_cells = conserved.shape
        steps = step_sizes(rows * radial_devices, wedge * phi_devices, theta_cells)
        radial_step, theta_step, phi_step, timestep = steps
        strength = GRAVITY_KICK / timestep
        own = wedge // SUBLANES
        assert rows == 8
        tiles, outer = own + 1, rows + 4
        zones = conserved.reshape(NV, rows, own, SUBLANES, theta_cells)
        position = lax.axis_index("radial").astype(jnp.int32).reshape(1)
        smem = pl.BlockSpec(memory_space=pltpu.SMEM)
        vmem = pl.BlockSpec(memory_space=pltpu.VMEM)
        hbm = pl.BlockSpec(memory_space=pl.ANY)
        f32 = jnp.float32
        limit = pltpu.CompilerParams(vmem_limit_bytes=VMEM_LIMIT)
        angle_scratch = pltpu.VMEM((4, SUBLANES, LANES), f32)

        def shape(*sizes):
            return jax.ShapeDtypeStruct(sizes, f32)

        def radius_at(index):
            return INNER_RADIUS + (splat(index) + 0.5) * radial_step

        def whole(value):
            return jnp.sum(value, axis=(0, 1), keepdims=True)

        side_rows = NV * rows * 4

        def pack(where, u, mass, wedge_before, wedge_after, to_chip, to_link):
            upper = 1 - lax.rem(where[0], 2)
            chip_start, link_start = (rows - 4) * upper, (rows - 4) * (1 - upper)
            sine = sine_of_zones(theta_step)
            lane = lane_index()
            tile = jnp.zeros((SUBLANES, LANES), f32)
            for r in range(rows):
                radius = radius_at((where[0] * rows + r).astype(f32))
                total = sum(u[0, r, t] for t in range(1, own)) + u[0, r, 0]
                shell = whole(total * sine) * (radius * radius * (radial_step * theta_step * phi_step))
                tile = jnp.where(lane == r, shell, tile)
            mass[...] = tile
            for k in range(NV):
                for r in range(rows):
                    at = (k * rows + r) * 4
                    wedge_before[at : at + 4] = u[k, r, 0, 0:4]
                    wedge_after[at : at + 4] = u[k, r, own - 1, 4:8]
                for r in range(4):
                    for t in range(own):
                        to_chip[k, r * own + t] = u[k, chip_start + r, t]
                        to_link[k, r * own + t] = u[k, link_start + r, t]

        slab = shape(NV, 4 * own, SUBLANES, LANES)
        corner = shape(NV, 2, SUBLANES, LANES)
        mass, wedge_before, wedge_after, to_chip, to_link = pl.pallas_call(
            pack,
            out_shape=[shape(8, LANES), shape(side_rows, LANES), shape(side_rows, LANES), slab, slab],
            in_specs=[smem, vmem],
            out_specs=[vmem] * 5,
            compiler_params=limit,
            name="pack",
        )(position, zones)

        wedge_low = lax.ppermute(wedge_after, "phi", clockwise)
        wedge_high = lax.ppermute(wedge_before, "phi", counter)
        from_chip = lax.ppermute(to_chip, "radial", chip)
        from_link = lax.ppermute(to_link, "radial", link)
        mass_beside = lax.ppermute(mass, "phi", pair)
        lanes = lax.broadcasted_iota(jnp.int32, (SUBLANES, LANES), 1)
        pair_mass = jnp.where(lanes == rows, core_mass[0], mass + mass_beside)
        rest_mass = lax.ppermute(pair_mass, "phi", pair_across)

        def add_wedges(mass, rest, masses):
            total = jnp.where(lane_index()[0:1] == rows, mass[0:1], mass[0:1] + rest[0:1])
            for peer in range(radial_devices):
                masses[peer] = total

        masses = pl.pallas_call(
            add_wedges,
            out_shape=shape(radial_devices, 1, LANES),
            in_specs=[vmem] * 2,
            out_specs=vmem,
            compiler_params=limit,
            name="add_wedges",
        )(pair_mass, rest_mass)

        everyone = lax.all_to_all(masses, "radial", 0, 0, tiled=True).reshape(radial_devices, LANES)

        def sides(where, low, high, h, to_chip, to_link):
            upper = 1 - lax.rem(where[0], 2)
            chip_start, link_start = (rows - 2) * upper, (rows - 2) * (1 - upper)
            for k in range(NV):
                for r in range(rows):
                    at = (k * rows + r) * 4
                    h[k, r, 0:4] = high[at : at + 4]
                    h[k, r, 4:8] = low[at : at + 4]
                for r in range(2):
                    to_chip[k, r] = h[k, chip_start + r]
                    to_link[k, r] = h[k, link_start + r]

        h, corner_to_chip, corner_to_link = pl.pallas_call(
            sides,
            out_shape=[shape(NV, rows, SUBLANES, LANES), corner, corner],
            in_specs=[smem] + [vmem] * 2,
            out_specs=[vmem] * 3,
            compiler_params=limit,
            name="sides",
        )(position, wedge_low, wedge_high)

        corner_from_chip = lax.ppermute(corner_to_chip, "radial", chip)
        corner_from_link = lax.ppermute(corner_to_link, "radial", link)

        block = 4

        def fill_window(x, outer_side, u, h, slab, corner):
            ours, theirs = block * (1 - outer_side), block * outer_side
            start = (rows - block) * outer_side
            near, far = theirs + 2 * (1 - outer_side), theirs + 2 * outer_side
            for k in range(NV):
                for r in range(block):
                    for t in range(own):
                        x[ours + r, k, t] = u[k, start + r, t]
                        x[theirs + r, k, t] = slab[k, r * own + t]
                    x[ours + r, k, own] = h[k, start + r]
                for r in range(2):
                    x[near + r, k, own] = corner[k, r]
                    x[far + r, k, own] = splat(1.0)

        def update_window(x, kept, angles, first, out, pulled, base):
            def emit(r, state, rate):
                for k in range(NV):
                    out[base + r, k] = state[k] + timestep * rate[k]
                pulled[base + r, 0] = jnp.maximum(state[0], MINIMUM_DENSITY)
                pulled[base + r, 1] = state[1]

            rate_rows(x, kept, angles, block, tiles, first, steps, UNROLL1, emit)

        def middle_rows(where, u, h, out, pulled, x, kept, angles):
            fill_angles(angles, steps)
            for k in range(NV):
                for r in range(rows):
                    for t in range(own):
                        x[r, k, t] = u[k, r, t]
                    x[r, k, own] = h[k, r]
            update_window(x, kept, angles, where[0] * rows + 2, out, pulled, 0)

        def edge_rows(where, outer_side, u, h, slab, corner, out, pulled, x, kept, angles, ends):
            fill_angles(angles, steps)
            fill_window(x, outer_side, u, h, slab, corner)
            if ends:

                @pl.when(where[0] == 0)
                def _():
                    for k in range(NV):
                        x[2, k] = x[4, k]
                        x[3, k] = x[4, k]

                @pl.when(where[0] == radial_devices - 1)
                def _():
                    for k in range(NV):
                        x[4, k] = x[3, k]
                        x[5, k] = x[3, k]

            first = where[0] * rows - 2 + rows * outer_side
            update_window(x, kept, angles, first, out, pulled, block * outer_side)

        def chip_rows(where, u, h, slab, corner, out, pulled, x, kept, angles):
            edge_rows(where, 1 - lax.rem(where[0], 2), u, h, slab, corner, out, pulled, x, kept, angles, False)

        def link_rows(where, u, h, slab, corner, _out, _pulled, out, pulled, x, kept, angles):
            edge_rows(where, lax.rem(where[0], 2), u, h, slab, corner, out, pulled, x, kept, angles, True)

        window = pltpu.VMEM((block + 4, NV, tiles, SUBLANES, LANES), f32)
        kept_scratch = pltpu.VMEM((3, NV, tiles, SUBLANES, LANES), f32)

        def section_shapes(count):
            return [shape(count, NV, tiles, SUBLANES, LANES), shape(count, 2, tiles, SUBLANES, LANES)]

        middle, middle_pulled = pl.pallas_call(
            middle_rows,
            out_shape=section_shapes(block),
            in_specs=[smem] + [vmem] * 2,
            out_specs=[vmem] * 2,
            scratch_shapes=[window, kept_scratch, angle_scratch],
            compiler_params=limit,
            name="middle_rows",
        )(position, zones, h)
        edge_call = dict(
            out_shape=section_shapes(2 * block),
            out_specs=[vmem] * 2,
            scratch_shapes=[window, kept_scratch, angle_scratch],
            compiler_params=limit,
        )
        edges, edges_pulled = pl.pallas_call(
            chip_rows, in_specs=[smem] + [vmem] * 4, name="chip_rows", **edge_call
        )(position, zones, h, from_chip, corner_from_chip)
        edges, edges_pulled = pl.pallas_call(
            link_rows,
            in_specs=[smem] + [vmem] * 6,
            input_output_aliases={5: 0, 6: 1},
            name="link_rows",
            **edge_call,
        )(position, zones, h, from_link, corner_from_link, edges, edges_pulled)

        def second_section(
            where, masses, u, middle, middle_pulled, edges, edges_pulled, out, enclosed,
            x, kept, angles, pulls, done, sent,
        ):
            fill_angles(angles, steps)
            first = where[0] * rows
            device = lax.broadcasted_iota(jnp.int32, (radial_devices, LANES), 0)
            lane = lax.broadcasted_iota(jnp.int32, (radial_devices, LANES), 1)
            zone = device * rows + lane
            shell = jnp.where(lane < rows, masses[...], 0.0)
            core = splat(1.0) * masses[0:1, rows : rows + 1]
            line = jnp.zeros((1, LANES), f32)
            for j in range(outer):
                index = first + (j - 2)
                weight = jnp.where(zone < index, 1.0, jnp.where(zone == index, 0.5, 0.0))
                inside = whole(shell * weight) + core
                radius = radius_at(index.astype(f32))
                pull = (timestep * strength) * inside / (radius * radius)
                pulls[j] = pull
                line = jnp.where(lane[0:1] == j - 2, inside[0:1], line)
                if j < block:
                    part, pulled, at = edges, edges_pulled, j
                elif j < 2 * block:
                    part, pulled, at = middle, middle_pulled, j - block
                else:
                    part, pulled, at = edges, edges_pulled, j - block
                for k in range(NV):
                    if k == 1:
                        x[j, k] = part[at, k] - pull * pulled[at, 0]
                    elif k == 4:
                        x[j, k] = part[at, k] - pull * pulled[at, 1]
                    else:
                        x[j, k] = part[at, k]
            enclosed[...] = line[:, :rows]
            fill_ends(x, rows, where[0], radial_devices - 1)

            def leave(r):
                return pltpu.make_async_copy(done.at[r], out.at[:, r], sent.at[r])

            def emit(r, state, rate):
                pull = pulls[r + 2]
                density = jnp.maximum(state[0], MINIMUM_DENSITY)
                for k in range(NV):
                    change = timestep * rate[k]
                    if k == 1:
                        change = change - pull * density
                    if k == 4:
                        change = change - pull * state[1]
                    done[r, k] = 0.5 * u[k, r] + 0.5 * (state[k] + change)
                leave(r).start()

            rate_rows(x, kept, angles, rows, own, first, steps, UNROLL2, emit)
            for r in range(rows):
                leave(r).wait()

        advanced, enclosed = pl.pallas_call(
            second_section,
            out_shape=[shape(*zones.shape), shape(1, rows)],
            in_specs=[smem] + [vmem] * 6,
            out_specs=[hbm, vmem],
            scratch_shapes=[
                pltpu.VMEM((outer, NV, tiles, SUBLANES, LANES), f32),
                pltpu.VMEM((3, NV, own, SUBLANES, LANES), f32),
                angle_scratch,
                pltpu.VMEM((outer, SUBLANES, LANES), f32),
                pltpu.VMEM((rows, NV, own, SUBLANES, LANES), f32),
                pltpu.SemaphoreType.DMA((rows,)),
            ],
            compiler_params=limit,
            name="second_section",
        )(position, everyone, zones, middle, middle_pulled, edges, edges_pulled)
        return advanced.reshape(conserved.shape), enclosed.reshape(rows)

    in_specs = (P(None, "radial", "phi", None), P())
    out_specs = (P(None, "radial", "phi", None), P("radial"))
    return jax.shard_map(step, mesh=mesh, in_specs=in_specs, out_specs=out_specs, check_vma=False)
```

```python
import math

import jax
import jax.numpy as jnp
from jax import lax
from jax.experimental import pallas as pl
from jax.experimental.pallas import tpu as pltpu
from jax.sharding import PartitionSpec as P

ADIABATIC = 4.0 / 3.0
INNER_RADIUS = 1.0
OUTER_RADIUS = 2.0
COURANT = 0.4
GRAVITY_KICK = 0.004
MINIMUM_DENSITY = 0.05
PRESSURE_FLOOR = 0.01
NV = 8
LANES = 128
SUBLANES = 8
UNROLL1 = 2
UNROLL2 = 4
VMEM_LIMIT = 12 * 1024 * 1024


def step_sizes(radial_total, phi_total, theta_total):
    theta_step = math.pi / theta_total
    phi_step = 2.0 * math.pi / phi_total
    polar_width = INNER_RADIUS * math.sin(0.5 * theta_step) * phi_step
    radial_step = min(2.0 * polar_width, (OUTER_RADIUS - INNER_RADIUS) / radial_total)
    timestep = COURANT * min(radial_step, polar_width)
    return (radial_step, theta_step, phi_step, timestep)


def splat(value):
    return jnp.full((SUBLANES, LANES), value, jnp.float32)


def lane_index():
    return lax.broadcasted_iota(jnp.int32, (SUBLANES, LANES), 1)


def sine_of_zones(theta_step):
    return jnp.sin((lane_index().astype(jnp.float32) + 0.5) * theta_step)


def fill_angles(angles, steps):
    _, theta_step, phi_step, _ = steps
    lane = lane_index().astype(jnp.float32)
    sine = sine_of_zones(theta_step)
    angles[0] = jnp.cos((lane + 0.5) * theta_step) / sine
    angles[1] = jnp.sin((lane + 1.0) * theta_step) * (0.5 / (sine * theta_step))
    angles[2] = jnp.sin(lane * theta_step) * (0.5 / (sine * theta_step))
    angles[3] = 0.5 / (sine * phi_step)


def half_slope(below, above):
    return 0.5 * jnp.maximum(jnp.minimum(above, jnp.maximum(below, 0.0)), jnp.minimum(below, 0.0))


def thermo(u):
    density = jnp.maximum(u[0], MINIMUM_DENSITY)
    inverse = 1.0 / density
    kinetic = (0.5 * inverse) * (u[1] * u[1] + u[2] * u[2] + u[3] * u[3])
    pressure = jnp.maximum((ADIABATIC - 1.0) * (u[4] - kinetic), PRESSURE_FLOOR * density)
    return density, inverse, pressure


def side(u, component):
    _, inverse, pressure = thermo(u)
    normal = u[component] * inverse
    square = (ADIABATIC * pressure) * inverse
    return normal, pressure, jnp.abs(normal) + square * lax.rsqrt(square)


def face_flux(left, right, component):
    vl, pl_, al = side(left, component)
    vr, pr, ar = side(right, component)
    signal = jnp.maximum(al, ar)
    toward, away = vl + signal, vr - signal
    out = [left[k] * toward + right[k] * away for k in range(NV)]
    out[component] = out[component] + (pl_ + pr)
    out[4] = out[4] + (pl_ * vl + pr * vr)
    return out


def next_zone(value, edge):
    turned = pltpu.roll(value, SUBLANES - 1, 1)
    return jnp.where(edge, jnp.concatenate([turned[1:], turned[:1]], axis=0), turned)


def previous_zone(value, edge):
    turned = pltpu.roll(value, 1, 1)
    return jnp.where(edge, jnp.concatenate([turned[-1:], turned[:-1]], axis=0), turned)


def rate_rows(x, kept, angles, rows, wide, first_row, steps, unroll, emit):
    radial_step = steps[0]

    def radius_of(index):
        return INNER_RADIUS + (splat(index) + 0.5) * radial_step

    def states(j, below):
        left, right, above = [], [], []
        for k in range(NV):
            centre = x[j, k, :wide]
            difference = x[j + 1, k, :wide] - centre
            slope = half_slope(below[k], difference)
            left.append(centre + slope)
            right.append(centre - slope)
            above.append(difference)
        return left, right, above

    def keep(left, above):
        for k in range(NV):
            kept[0, k] = left[k]
            kept[1, k] = above[k]

    def radial_face(f):
        inner = [kept[0, k] for k in range(NV)]
        left, right, above = states(f + 2, [kept[1, k] for k in range(NV)])
        keep(left, above)
        face = radius_of(jnp.asarray(first_row + f).astype(jnp.float32)) - 0.5 * radial_step
        area = (0.5 / radial_step) * face * face
        return [area * value for value in face_flux(inner, right, 1)]

    left, _, above = states(1, [x[1, k, :wide] - x[0, k, :wide] for k in range(NV)])
    keep(left, above)
    for k, value in enumerate(radial_face(0)):
        kept[2, k] = value

    last = lane_index() == LANES - 1
    sublane = lax.broadcasted_iota(jnp.int32, (SUBLANES, LANES), 0)
    top, bottom = sublane == SUBLANES - 1, sublane == 0

    def row(r, carry):
        inverse_radius = 1.0 / radius_of((first_row + r).astype(jnp.float32))
        radial_scale = inverse_radius * inverse_radius
        u = [x[r + 2, k, :wide] for k in range(NV)]
        upper = radial_face(r + 1)
        rate = [(kept[2, k] - upper[k]) * radial_scale for k in range(NV)]
        for k in range(NV):
            kept[2, k] = upper[k]
        left, right = [], []
        for k in range(NV):
            after = jnp.where(last, u[k], pltpu.roll(u[k], LANES - 1, 2))
            above = after - u[k]
            slope = half_slope(pltpu.roll(above, 1, 2), above)
            left.append(u[k] + slope)
            right.append(after - pltpu.roll(slope, LANES - 1, 2))
        flux = face_flux(left, right, 2)
        upper, lower = angles[1] * inverse_radius, angles[2] * inverse_radius
        for k in range(NV):
            rate[k] = rate[k] - (upper * flux[k] - lower * pltpu.roll(flux[k], 1, 2))
        left, right = [], []
        for k in range(NV):
            zones = x[r + 2, k]
            after = next_zone(zones, top)
            above = after - zones
            slope = half_slope(previous_zone(above, bottom), above)
            left.append(zones + slope)
            right.append(after - next_zone(slope, top))
        flux = face_flux(left, right, 3)
        scale = angles[3] * inverse_radius
        for k in range(NV):
            rate[k] = rate[k] - scale * (flux[k][:wide] - previous_zone(flux[k], bottom)[:wide])
        density, inverse, pressure = thermo(u)
        cotangent = angles[0]
        vr, vt, vp = u[1] * inverse, u[2] * inverse, u[3] * inverse
        azimuth_push = density * vp * vp
        polar_carry = density * vt
        rate[1] = rate[1] + (2.0 * pressure + (polar_carry * vt + azimuth_push)) * inverse_radius
        rate[2] = rate[2] + ((pressure + azimuth_push) * cotangent - polar_carry * vr) * inverse_radius
        rate[3] = rate[3] - density * vp * (vr + vt * cotangent) * inverse_radius
        emit(r, u, rate)
        return carry

    lax.fori_loop(0, rows, row, 0, unroll=unroll)


def fill_ends(x, rows, position, last_position):
    first = (x.shape[0] - rows) // 2
    last = first + rows - 1

    @pl.when(position == 0)
    def _():
        for k in range(NV):
            x[first - 2, k] = x[first, k]
            x[first - 1, k] = x[first, k]

    @pl.when(position == last_position)
    def _():
        for k in range(NV):
            x[last + 1, k] = x[last, k]
            x[last + 2, k] = x[last, k]


def solution(mesh):
    radial_devices, phi_devices = mesh.shape["radial"], mesh.shape["phi"]
    assert phi_devices == 4 and radial_devices % 2 == 0
    chip = [(i, i ^ 1) for i in range(radial_devices)]
    link = [(i, min(max(i + (1 if i % 2 else -1), 0), radial_devices - 1)) for i in range(radial_devices)]
    clockwise = [(i, (i + 1) % phi_devices) for i in range(phi_devices)]
    counter = [(j, i) for i, j in clockwise]
    pair = [(0, 1), (1, 0), (2, 3), (3, 2)]
    pair_across = [(0, 3), (3, 0), (1, 2), (2, 1)]

    def step(conserved, core_mass):
        _, rows, wedge, theta_cells = conserved.shape
        steps = step_sizes(rows * radial_devices, wedge * phi_devices, theta_cells)
        radial_step, theta_step, phi_step, timestep = steps
        strength = GRAVITY_KICK / timestep
        own = wedge // SUBLANES
        assert rows == 8
        tiles, outer = own + 1, rows + 4
        zones = conserved.reshape(NV, rows, own, SUBLANES, theta_cells)
        position = lax.axis_index("radial").astype(jnp.int32).reshape(1)
        smem = pl.BlockSpec(memory_space=pltpu.SMEM)
        vmem = pl.BlockSpec(memory_space=pltpu.VMEM)
        hbm = pl.BlockSpec(memory_space=pl.ANY)
        f32 = jnp.float32
        limit = pltpu.CompilerParams(vmem_limit_bytes=VMEM_LIMIT)
        angle_scratch = pltpu.VMEM((4, SUBLANES, LANES), f32)

        def shape(*sizes):
            return jax.ShapeDtypeStruct(sizes, f32)

        def radius_at(index):
            return INNER_RADIUS + (splat(index) + 0.5) * radial_step

        def whole(value):
            return jnp.sum(value, axis=(0, 1), keepdims=True)

        side_rows = NV * rows * 4

        def pack(where, far, mass, wedge_before, wedge_after, to_chip, to_link, u, arrived):
            def fetch(k):
                return pltpu.make_async_copy(far.at[k], u.at[k], arrived.at[k])

            for k in range(NV):
                fetch(k).start()
            fetch(0).wait()
            upper = 1 - lax.rem(where[0], 2)
            chip_start, link_start = (rows - 4) * upper, (rows - 4) * (1 - upper)
            sine = sine_of_zones(theta_step)
            lane = lane_index()
            tile = jnp.zeros((SUBLANES, LANES), f32)
            for r in range(rows):
                radius = radius_at((where[0] * rows + r).astype(f32))
                total = sum(u[0, r, t] for t in range(1, own)) + u[0, r, 0]
                shell = whole(total * sine) * (radius * radius * (radial_step * theta_step * phi_step))
                tile = jnp.where(lane == r, shell, tile)
            mass[...] = tile
            for k in range(NV):
                if k:
                    fetch(k).wait()
                for r in range(rows):
                    at = (k * rows + r) * 4
                    wedge_before[at : at + 4] = u[k, r, 0, 0:4]
                    wedge_after[at : at + 4] = u[k, r, own - 1, 4:8]
                for r in range(4):
                    for t in range(own):
                        to_chip[k, r * own + t] = u[k, chip_start + r, t]
                        to_link[k, r * own + t] = u[k, link_start + r, t]

        slab = shape(NV, 4 * own, SUBLANES, LANES)
        corner = shape(NV, 2, SUBLANES, LANES)
        mass, wedge_before, wedge_after, to_chip, to_link = pl.pallas_call(
            pack,
            out_shape=[shape(8, LANES), shape(side_rows, LANES), shape(side_rows, LANES), slab, slab],
            in_specs=[smem, pl.BlockSpec(memory_space=pltpu.HBM)],
            scratch_shapes=[
                pltpu.VMEM((NV, rows, own, SUBLANES, theta_cells), f32),
                pltpu.SemaphoreType.DMA((NV,)),
            ],
            out_specs=[vmem] * 5,
            compiler_params=limit,
            name="pack",
        )(position, pltpu.with_memory_space_constraint(zones, pltpu.HBM))

        wedge_low = lax.ppermute(wedge_after, "phi", clockwise)
        wedge_high = lax.ppermute(wedge_before, "phi", counter)
        from_chip = lax.ppermute(to_chip, "radial", chip)
        from_link = lax.ppermute(to_link, "radial", link)
        mass_beside = lax.ppermute(mass, "phi", pair)
        lanes = lax.broadcasted_iota(jnp.int32, (SUBLANES, LANES), 1)
        pair_mass = jnp.where(lanes == rows, core_mass[0], mass + mass_beside)
        rest_mass = lax.ppermute(pair_mass, "phi", pair_across)

        def add_wedges(mass, rest, masses):
            total = jnp.where(lane_index()[0:1] == rows, mass[0:1], mass[0:1] + rest[0:1])
            for peer in range(radial_devices):
                masses[peer] = total

        masses = pl.pallas_call(
            add_wedges,
            out_shape=shape(radial_devices, 1, LANES),
            in_specs=[vmem] * 2,
            out_specs=vmem,
            compiler_params=limit,
            name="add_wedges",
        )(pair_mass, rest_mass)

        everyone = lax.all_to_all(masses, "radial", 0, 0, tiled=True).reshape(radial_devices, LANES)

        def sides(where, low, high, h, to_chip, to_link):
            upper = 1 - lax.rem(where[0], 2)
            chip_start, link_start = (rows - 2) * upper, (rows - 2) * (1 - upper)
            for k in range(NV):
                for r in range(rows):
                    at = (k * rows + r) * 4
                    h[k, r, 0:4] = high[at : at + 4]
                    h[k, r, 4:8] = low[at : at + 4]
                for r in range(2):
                    to_chip[k, r] = h[k, chip_start + r]
                    to_link[k, r] = h[k, link_start + r]

        h, corner_to_chip, corner_to_link = pl.pallas_call(
            sides,
            out_shape=[shape(NV, rows, SUBLANES, LANES), corner, corner],
            in_specs=[smem] + [vmem] * 2,
            out_specs=[vmem] * 3,
            compiler_params=limit,
            name="sides",
        )(position, wedge_low, wedge_high)

        corner_from_chip = lax.ppermute(corner_to_chip, "radial", chip)
        corner_from_link = lax.ppermute(corner_to_link, "radial", link)

        block = 4

        def fill_window(x, outer_side, u, h, slab, corner):
            ours, theirs = block * (1 - outer_side), block * outer_side
            start = (rows - block) * outer_side
            near, far = theirs + 2 * (1 - outer_side), theirs + 2 * outer_side
            for k in range(NV):
                for r in range(block):
                    for t in range(own):
                        x[ours + r, k, t] = u[k, start + r, t]
                        x[theirs + r, k, t] = slab[k, r * own + t]
                    x[ours + r, k, own] = h[k, start + r]
                for r in range(2):
                    x[near + r, k, own] = corner[k, r]
                    x[far + r, k, own] = splat(1.0)

        def update_window(x, kept, angles, first, out, pulled, base):
            def emit(r, state, rate):
                for k in range(NV):
                    out[base + r, k] = state[k] + timestep * rate[k]
                pulled[base + r, 0] = jnp.maximum(state[0], MINIMUM_DENSITY)
                pulled[base + r, 1] = state[1]

            rate_rows(x, kept, angles, block, tiles, first, steps, UNROLL1, emit)

        def middle_rows(where, u, h, out, pulled, x, kept, angles):
            fill_angles(angles, steps)
            for k in range(NV):
                for r in range(rows):
                    for t in range(own):
                        x[r, k, t] = u[k, r, t]
                    x[r, k, own] = h[k, r]
            update_window(x, kept, angles, where[0] * rows + 2, out, pulled, 0)

        def edge_rows(where, outer_side, u, h, slab, corner, out, pulled, x, kept, angles, ends):
            fill_angles(angles, steps)
            fill_window(x, outer_side, u, h, slab, corner)
            if ends:

                @pl.when(where[0] == 0)
                def _():
                    for k in range(NV):
                        x[2, k] = x[4, k]
                        x[3, k] = x[4, k]

                @pl.when(where[0] == radial_devices - 1)
                def _():
                    for k in range(NV):
                        x[4, k] = x[3, k]
                        x[5, k] = x[3, k]

            first = where[0] * rows - 2 + rows * outer_side
            update_window(x, kept, angles, first, out, pulled, block * outer_side)

        def chip_rows(where, u, h, slab, corner, out, pulled, x, kept, angles):
            edge_rows(where, 1 - lax.rem(where[0], 2), u, h, slab, corner, out, pulled, x, kept, angles, False)

        def link_rows(where, u, h, slab, corner, _out, _pulled, out, pulled, x, kept, angles):
            edge_rows(where, lax.rem(where[0], 2), u, h, slab, corner, out, pulled, x, kept, angles, True)

        window = pltpu.VMEM((block + 4, NV, tiles, SUBLANES, LANES), f32)
        kept_scratch = pltpu.VMEM((3, NV, tiles, SUBLANES, LANES), f32)

        def section_shapes(count):
            return [shape(count, NV, tiles, SUBLANES, LANES), shape(count, 2, tiles, SUBLANES, LANES)]

        middle, middle_pulled = pl.pallas_call(
            middle_rows,
            out_shape=section_shapes(block),
            in_specs=[smem] + [vmem] * 2,
            out_specs=[vmem] * 2,
            scratch_shapes=[window, kept_scratch, angle_scratch],
            compiler_params=limit,
            name="middle_rows",
        )(position, zones, h)
        edge_call = dict(
            out_shape=section_shapes(2 * block),
            out_specs=[vmem] * 2,
            scratch_shapes=[window, kept_scratch, angle_scratch],
            compiler_params=limit,
        )
        edges, edges_pulled = pl.pallas_call(
            chip_rows, in_specs=[smem] + [vmem] * 4, name="chip_rows", **edge_call
        )(position, zones, h, from_chip, corner_from_chip)
        edges, edges_pulled = pl.pallas_call(
            link_rows,
            in_specs=[smem] + [vmem] * 6,
            input_output_aliases={5: 0, 6: 1},
            name="link_rows",
            **edge_call,
        )(position, zones, h, from_link, corner_from_link, edges, edges_pulled)

        def second_section(
            where, masses, u, middle, middle_pulled, edges, edges_pulled, out, enclosed,
            x, kept, angles, pulls, done, sent,
        ):
            fill_angles(angles, steps)
            first = where[0] * rows
            device = lax.broadcasted_iota(jnp.int32, (radial_devices, LANES), 0)
            lane = lax.broadcasted_iota(jnp.int32, (radial_devices, LANES), 1)
            zone = device * rows + lane
            shell = jnp.where(lane < rows, masses[...], 0.0)
            core = splat(1.0) * masses[0:1, rows : rows + 1]
            line = jnp.zeros((1, LANES), f32)
            for j in range(outer):
                index = first + (j - 2)
                weight = jnp.where(zone < index, 1.0, jnp.where(zone == index, 0.5, 0.0))
                inside = whole(shell * weight) + core
                radius = radius_at(index.astype(f32))
                pull = (timestep * strength) * inside / (radius * radius)
                pulls[j] = pull
                line = jnp.where(lane[0:1] == j - 2, inside[0:1], line)
                if j < block:
                    part, pulled, at = edges, edges_pulled, j
                elif j < 2 * block:
                    part, pulled, at = middle, middle_pulled, j - block
                else:
                    part, pulled, at = edges, edges_pulled, j - block
                for k in range(NV):
                    if k == 1:
                        x[j, k] = part[at, k] - pull * pulled[at, 0]
                    elif k == 4:
                        x[j, k] = part[at, k] - pull * pulled[at, 1]
                    else:
                        x[j, k] = part[at, k]
            enclosed[...] = line[:, :rows]
            fill_ends(x, rows, where[0], radial_devices - 1)

            def leave(r):
                return pltpu.make_async_copy(done.at[r], out.at[:, r], sent.at[r])

            def emit(r, state, rate):
                pull = pulls[r + 2]
                density = jnp.maximum(state[0], MINIMUM_DENSITY)
                for k in range(NV):
                    change = timestep * rate[k]
                    if k == 1:
                        change = change - pull * density
                    if k == 4:
                        change = change - pull * state[1]
                    done[r, k] = 0.5 * u[k, r] + 0.5 * (state[k] + change)
                leave(r).start()

            rate_rows(x, kept, angles, rows, own, first, steps, UNROLL2, emit)
            for r in range(rows):
                leave(r).wait()

        advanced, enclosed = pl.pallas_call(
            second_section,
            out_shape=[shape(*zones.shape), shape(1, rows)],
            in_specs=[smem] + [vmem] * 6,
            out_specs=[hbm, vmem],
            scratch_shapes=[
                pltpu.VMEM((outer, NV, tiles, SUBLANES, LANES), f32),
                pltpu.VMEM((3, NV, own, SUBLANES, LANES), f32),
                angle_scratch,
                pltpu.VMEM((outer, SUBLANES, LANES), f32),
                pltpu.VMEM((rows, NV, own, SUBLANES, LANES), f32),
                pltpu.SemaphoreType.DMA((rows,)),
            ],
            compiler_params=limit,
            name="second_section",
        )(position, everyone, zones, middle, middle_pulled, edges, edges_pulled)
        return advanced.reshape(conserved.shape), enclosed.reshape(rows)

    in_specs = (P(None, "radial", "phi", None), P())
    out_specs = (P(None, "radial", "phi", None), P("radial"))
    return jax.shard_map(step, mesh=mesh, in_specs=in_specs, out_specs=out_specs, check_vma=False)
```
